32 devices in a mesh: vocab: 8 (over y, x, core), seq: 4 (over z).
Axes of the slice: x: 2, y: 2, z: 4, core: 2. Of those that a mesh axis runs over, the one named last changes fastest.
Arguments:
- latent_vector: bfloat16 [32, 7168], P('vocab', 'seq'), may hold values from -400 to 400
- unembedding_matrix: bfloat16 [7168, 8192], P('seq', 'vocab'), may hold values from -0.0625 to 0.0625
- occurrence_tally: int32 [32, 8192], P(('seq', 'vocab')), may hold values from 0 to 2
- additive_offset_table: bfloat16 [32, 8192], P(('seq', 'vocab')), may hold values from 0 to 0.5
- recurrence_charge: float32 [32], P(('seq', 'vocab')), may hold values from 0.05 to 0.5
- appearance_charge: float32 [32], P(('seq', 'vocab')), may hold values from 0.6 to 1.5
- recurrence_divisor: float32 [32], P('seq'), may hold values from 1.05 to 1.6
- softening_divisor: float32 [32], P('seq'), may hold values from 0.5 to 1.5
- nucleus_share_limit: float32 [32], P('seq'), may hold values from 0.5 to 0.95
Outputs:
- penalized_logits: bfloat16 [32, 8192], P('seq', 'vocab')
- cutoff: float32 [32], P('seq')
The draws below stay inside these ranges and needn't reach their ends.
Inputs may be any that keep to these rules, and one draw needn't show every extreme that they name: `appearance_charge`: each sequence's presence penalty exceeds every entry of its token bias.
All inputs are finite; a program needn't handle non-finite values.
Results may differ from the reference program's by a relative error of at most 0.0047.
Values may be sent and summed in bfloat16 or wider, within the bound.
No kernel may reach another device: no remote copies, remote signals or barrier semaphores. Data moves between devices by JAX's collectives and lax.ppermute only.
A program may use at most 64 MiB of HBM per device.

```python
import math
import jax
import jax.numpy as jnp
from jax import lax

D = 7168
STEPS = 9
STRAND_COUNT = 32
VOCAB = 8192


def draw_latent_vector(key, part):
    normal_part = jax.random.normal(jax.random.fold_in(key, 11), (STRAND_COUNT, D), jnp.float32)
    return jnp.clip(normal_part, -400.0, 400.0).astype(jnp.bfloat16)


def set_ends(result, own_key, least, high):
    longest = result.shape.index(max(result.shape))
    spots = []
    for shift in (0, 1):
        where = [jax.random.randint(jax.random.fold_in(own_key, axis), (), 0, length) for axis, length in enumerate(result.shape)]
        where[longest] = (where[longest] + shift) % result.shape[longest]
        spots.append(tuple(where))
    return result.at[spots[0]].set(least).at[spots[1]].set(high)


def levels(rng, shape, cuts, low, largest):
    def one(dim, parts):
        draws = jax.random.uniform(jax.random.fold_in(jax.random.fold_in(rng, 6), dim), (parts,), jnp.float32, low / len(cuts), largest / len(cuts))
        return jnp.repeat(jnp.exp(draws), shape[dim] // parts).reshape((-1,) + (1,) * (len(shape) - dim - 1))

    factor_of = one(*cuts[0])
    for cut in cuts[1:]:
        factor_of = factor_of * one(*cut)
    return factor_of


def noise(rng, shape, deviation, reach, cuts=(), held_as=jnp.bfloat16):
    gain = levels(rng, shape, cuts, -0.22, 0.18) if cuts else 1.0
    array = jax.random.normal(rng, shape, jnp.float32) * deviation * gain
    return jnp.minimum(jnp.maximum(array, -reach), reach).astype(held_as)


def setup_inputs(seed: int = 0) -> dict:
    streams_of = jax.random.split(jax.random.key(seed), 10)
    latent_vector = draw_latent_vector(jax.random.fold_in(streams_of[9], 71), 0)
    unembedding_matrix = noise(streams_of[1], (D, VOCAB), D ** -0.5, 0.0625, ((0, 4), (1, 8)))
    occurrence_tally = set_ends(jax.random.randint(streams_of[2], (STRAND_COUNT, VOCAB), 0, 3), jax.random.fold_in(streams_of[2], 1), 0, 2).astype(jnp.int32)
    additive_offset_table = jnp.clip(0.5 * jax.random.uniform(streams_of[3], (STRAND_COUNT, VOCAB), jnp.float32) ** levels(streams_of[3], (STRAND_COUNT, VOCAB), ((0, 32),), -0.2, 0.2), 0.0, 0.5).astype(jnp.bfloat16)
    recurrence_charge = jnp.clip(jnp.exp(math.log(0.5) - 2.3025851 * jax.random.uniform(streams_of[4], (STRAND_COUNT,), jnp.float32) ** levels(streams_of[4], (STRAND_COUNT,), ((0, 32),), -0.2, 0.2)), 0.05, 0.5)
    appearance_charge = jnp.clip(jnp.exp(math.log(1.5) - 0.9162907 * jax.random.uniform(streams_of[5], (STRAND_COUNT,), jnp.float32) ** levels(streams_of[5], (STRAND_COUNT,), ((0, 32),), -0.2, 0.2)), 0.6, 1.5)
    recurrence_divisor = jnp.clip(jnp.exp(math.log(1.6) - 0.42121353 * jax.random.uniform(streams_of[6], (STRAND_COUNT,), jnp.float32) ** levels(streams_of[6], (STRAND_COUNT,), ((0, 4),), -0.2, 0.2)), 1.05, 1.6)
    softening_divisor = jnp.clip(jnp.exp(math.log(1.5) - 1.0986123 * jax.random.uniform(streams_of[7], (STRAND_COUNT,), jnp.float32) ** levels(streams_of[7], (STRAND_COUNT,), ((0, 4),), -0.2, 0.2)), 0.5, 1.5)
    nucleus_share_limit = jnp.clip(0.5 + 0.45 * jax.random.uniform(streams_of[8], (STRAND_COUNT,), jnp.float32) ** levels(streams_of[8], (STRAND_COUNT,), ((0, 4),), -0.2, 0.2), 0.5, 0.95)
    return dict(latent_vector=latent_vector, unembedding_matrix=unembedding_matrix, occurrence_tally=occurrence_tally, additive_offset_table=additive_offset_table, recurrence_charge=recurrence_charge, appearance_charge=appearance_charge, recurrence_divisor=recurrence_divisor, softening_divisor=softening_divisor, nucleus_share_limit=nucleus_share_limit)


cutoff_span = 32.0


def reference(latent_vector, unembedding_matrix, occurrence_tally, additive_offset_table, recurrence_charge, appearance_charge, recurrence_divisor, softening_divisor, nucleus_share_limit):
    logits = jnp.dot(latent_vector, unembedding_matrix, preferred_element_type=jnp.float32)
    count_float = occurrence_tally.astype(jnp.float32)
    seen_mask = occurrence_tally > 0
    offset = (additive_offset_table.astype(jnp.float32) - recurrence_charge[:, None] * count_float
              - appearance_charge[:, None] * seen_mask.astype(jnp.float32)).astype(jnp.bfloat16)
    factor = recurrence_divisor[:, None]
    discouraged_scores = jnp.where(seen_mask, jnp.where(logits > 0, logits / factor, logits * factor), logits) + offset.astype(jnp.float32)
    softened_scores = discouraged_scores / softening_divisor[:, None]
    largest_score = jnp.max(softened_scores, axis=1)
    exponential_values = jnp.exp(softened_scores - largest_score[:, None])
    row_total = jnp.sum(exponential_values, axis=1)
    target = nucleus_share_limit * row_total

    def bisect_step(turn_index, bounds):
        lower_end, upper_end = bounds
        middle = (lower_end + upper_end) * 0.5
        threshold_candidates = largest_score - cutoff_span * middle
        cumulative_shares = jnp.sum(jnp.where(softened_scores >= threshold_candidates[:, None], exponential_values, 0.0), axis=1)
        below_mask = cumulative_shares < target
        return jnp.where(below_mask, middle, lower_end), jnp.where(below_mask, upper_end, middle)

    start_bounds = (jnp.zeros_like(largest_score), jnp.ones_like(largest_score))
    lower_end, upper_end = lax.fori_loop(0, STEPS, bisect_step, start_bounds)
    return discouraged_scores.astype(jnp.bfloat16), largest_score - cutoff_span * upper_end
```

```python
import jax
import jax.numpy as jnp
from jax import lax
from jax.sharding import PartitionSpec as P

STEPS = 9


cutoff_span = 32.0


def per_device(
    latent_vector,
    unembedding_matrix,
    occurrence_tally,
    additive_offset_table,
    recurrence_charge,
    appearance_charge,
    recurrence_divisor,
    softening_divisor,
    nucleus_share_limit,
):
    vocab_parts = lax.axis_size("vocab")
    seq_parts = lax.axis_size("seq")
    own_rows, vocab = occurrence_tally.shape
    block = unembedding_matrix.shape[1]

    def own(vector):
        return lax.dynamic_slice_in_dim(vector, lax.axis_index("vocab") * own_rows, own_rows, 0)

    factor = own(recurrence_divisor)[:, None]
    softening = own(softening_divisor)[:, None]
    share = own(nucleus_share_limit)

    seen_mask = occurrence_tally > 0
    offset = lax.reduce_precision(
        additive_offset_table.astype(jnp.float32)
        - recurrence_charge[:, None] * occurrence_tally.astype(jnp.float32)
        - appearance_charge[:, None] * seen_mask.astype(jnp.float32),
        exponent_bits=8,
        mantissa_bits=7,
    )

    partial_logits = jnp.dot(
        lax.all_gather(latent_vector, "vocab", axis=0, tiled=True),
        unembedding_matrix,
        preferred_element_type=jnp.float32,
    )
    pieces = partial_logits.reshape(seq_parts * vocab_parts, own_rows, block)
    pieces = lax.all_to_all(pieces, ("seq", "vocab"), split_axis=0, concat_axis=0, tiled=True)
    pieces = pieces.reshape(seq_parts, vocab_parts, own_rows, block).sum(axis=0)
    logits = pieces.transpose(1, 0, 2).reshape(own_rows, vocab)

    discouraged_scores = jnp.where(
        seen_mask, jnp.where(logits > 0, logits / factor, logits * factor), logits
    ) + offset
    softened_scores = discouraged_scores / softening
    largest_score = jnp.max(softened_scores, axis=1)
    exponential_values = jnp.exp(softened_scores - largest_score[:, None])
    target = share * jnp.sum(exponential_values, axis=1)
    lower_end = jnp.zeros_like(largest_score)
    upper_end = jnp.ones_like(largest_score)
    fractions = jnp.arange(1, 8, dtype=jnp.float32)
    for _ in range(STEPS // 3):
        stride = (upper_end - lower_end) * 0.125
        probes = lower_end[:, None] + stride[:, None] * fractions[None, :]
        threshold_candidates = largest_score[:, None] - cutoff_span * probes
        inside = softened_scores[:, None, :] >= threshold_candidates[:, :, None]
        mass = jnp.sum(jnp.where(inside, exponential_values[:, None, :], 0.0), axis=2)
        below_count = jnp.sum((mass < target[:, None]).astype(jnp.float32), axis=1)
        lower_end = lower_end + stride * below_count
        upper_end = lower_end + stride
    cutoff = largest_score - cutoff_span * upper_end

    blocks = discouraged_scores.reshape(own_rows, vocab_parts, block).transpose(1, 0, 2)
    beside = jnp.broadcast_to(cutoff[None, :, None], (vocab_parts, own_rows, 128))
    packed = jnp.concatenate([blocks, beside], axis=2)
    packed = lax.all_to_all(packed, "vocab", split_axis=0, concat_axis=0, tiled=True)
    packed = packed.reshape(vocab_parts * own_rows, block + 128)
    return packed[:, :block].astype(jnp.bfloat16), packed[:, block]


def solution(mesh):
    in_specs = (
        P("vocab", "seq"),
        P("seq", "vocab"),
        P(("seq", "vocab"), None),
        P(("seq", "vocab"), None),
        P(("seq", "vocab")),
        P(("seq", "vocab")),
        P("seq"),
        P("seq"),
        P("seq"),
    )
    out_specs = (P("seq", "vocab"), P("seq"))
    return jax.shard_map(
        per_device, mesh=mesh, in_specs=in_specs, out_specs=out_specs, check_vma=False
    )
```
